32 devices in a mesh: wide: 8 (over z, x), narrow: 4 (over y, core).
Axes of the slice: x: 2, y: 2, z: 4, core: 2. Of those that a mesh axis runs over, the one named last changes fastest.
Arguments:
- table: bfloat16 [32768, 512], P(('wide', 'narrow')), may hold values from -1.5 to 1.5
- relations: bfloat16 [7424, 512], replicated, may hold values from -6 to 6
- req_rows: int32 [32, 512], P(('wide', 'narrow')), may hold values from 0 to 1023, as said below
- owner_count: int32 [32, 32], P(('wide', 'narrow')), may hold values from 1 to 16, as said below
- owner_start: int32 [32, 32], P(('wide', 'narrow')), may hold values from 0 to 496, as said below
- head_slot: int32 [32768], P(('wide', 'narrow')), may hold values from 0 to 511, as said below
- rel_id: int32 [32768], P(('wide', 'narrow')), may hold values from 0 to 7423
- tail_slot: int32 [32768], P(('wide', 'narrow')), may hold values from 0 to 511, as said below
- neg_slot: int32 [32768], P(('wide', 'narrow')), may hold values from 0 to 511, as said below
Outputs:
- table_grad: float32 [32768, 512], P(('wide', 'narrow'))
The draws below stay inside these ranges and needn't reach their ends.
Inputs may be any that keep to these rules, and one draw needn't show every extreme that they name: `req_rows`: entries past the device's total of owner_count are ignored. A row may be asked more than once by one device of one owner; the gradients of all its slots add. `owner_count`: in every draw some owners receive exactly 16 rows from every device, and some device asks 16 rows of every owner. `owner_start`: the running sum of owner_count along owners, starting at 0. `head_slot`: below the device's total of owner_count. `tail_slot`: below the device's total of owner_count. `neg_slot`: below the device's total of owner_count.
All inputs are finite; a program needn't handle non-finite values.
Results may differ from the reference program's by a relative error of at most 0.0065.
Values may be sent and summed in bfloat16 or wider, within the bound.
No kernel may reach another device: no remote copies, remote signals or barrier semaphores. Data moves between devices by JAX's collectives and lax.ppermute only.
A program may use at most 64 MiB of HBM per device.

```python
import math
import jax
import jax.numpy as jnp
import numpy as np
from jax import lax

D = 512
NREL = 7424
ENT_DEV = 1024
B_DEV = 1024
NEG = 1024
CAP = 16
OWNERS = 32
SLOTS = 512
ENTITIES = 32768


def layout(key):
    base = jax.random.fold_in(key, 7001)
    hot = jax.random.randint(jax.random.fold_in(base, 1), (4,), 0, OWNERS)
    counts = jax.random.randint(jax.random.fold_in(base, 2), (OWNERS, OWNERS), 1, CAP // 2 + 1)
    is_hot = jnp.any(jnp.arange(OWNERS)[:, None] == hot[None, :], axis=1)
    counts = jnp.where(is_hot[None, :], CAP, counts)
    filled = jax.random.randint(jax.random.fold_in(base, 3), (), 0, OWNERS)
    is_full = jnp.arange(OWNERS)[:, None] == filled
    counts = jnp.where(is_full, CAP, counts).astype(jnp.int32)
    starts = (jnp.cumsum(counts, axis=1) - counts).astype(jnp.int32)
    totals = jnp.sum(counts, axis=1).astype(jnp.int32)
    return (counts, starts, totals)


def draw_req_rows(key, part):
    return jax.random.randint(jax.random.fold_in(key, 7101), (OWNERS, SLOTS), 0, ENT_DEV).astype(jnp.int32)


def draw_owner_count(key, part):
    return layout(key)[0]


def draw_owner_start(key, part):
    return layout(key)[1]


def draw_slots(key, salt, width):
    totals = layout(key)[2]
    picks = jax.random.randint(jax.random.fold_in(key, salt), (OWNERS, width), 0, totals[:, None])
    places = jax.random.randint(jax.random.fold_in(key, salt + 50), (OWNERS, 1), 0, width)
    column = jnp.arange(width)[None, :]
    picks = jnp.where(column == places, totals[:, None] - 1, picks)
    return picks.reshape(-1).astype(jnp.int32)


def draw_head_slot(key, part):
    return draw_slots(key, 7201, B_DEV)


def draw_tail_slot(key, part):
    return draw_slots(key, 7202, B_DEV)


def draw_neg_slot(key, part):
    return draw_slots(key, 7203, NEG)


def touch_ends(values, key, smallest, largest):
    longest = values.shape.index(max(values.shape))
    spots = []
    for shift in (0, 1):
        where = [jax.random.randint(jax.random.fold_in(key, axis), (), 0, length) for axis, length in enumerate(values.shape)]
        where[longest] = (where[longest] + shift) % values.shape[longest]
        spots.append(tuple(where))
    return values.at[spots[0]].set(smallest).at[spots[1]].set(largest)


def steps_of(key, shape, split, low, high):
    def one(axis_at, blocks):
        steps = jax.random.uniform(jax.random.fold_in(jax.random.fold_in(key, 6), axis_at), (blocks,), jnp.float32, low / len(split), high / len(split))
        return jnp.repeat(jnp.exp(steps), shape[axis_at] // blocks).reshape((-1,) + (1,) * (len(shape) - axis_at - 1))

    factor_of = one(*split[0])
    for cut in split[1:]:
        factor_of = factor_of * one(*cut)
    return factor_of


def rank_table(number_of, lean):
    loads = [(1 << 20) // math.isqrt(standing ** lean) + 1 for standing in range(1, number_of + 1)]
    deviation = 1 + sum(loads) // (1 << 30)
    return np.cumsum(np.array([max(1, weight // deviation) for weight in loads]))


def ranked(own_key, shape, amount, lean):
    grid = rank_table(amount, lean)
    lot = jax.random.randint(jax.random.fold_in(own_key, 1), shape, 0, int(grid[amount - 1]))
    standing = jnp.searchsorted(jnp.asarray(grid, jnp.int32), lot, side="right")
    return jax.random.permutation(jax.random.fold_in(own_key, 2), amount)[standing].astype(jnp.int32)


def scatter_about(own_key, dims, deviation, reach, pieces=(), held_as=jnp.bfloat16):
    gain = steps_of(own_key, dims, pieces, -0.22, 0.18) if pieces else 1.0
    result = jax.random.normal(own_key, dims, jnp.float32) * deviation * gain
    return jnp.minimum(jnp.maximum(result, -reach), reach).astype(held_as)


def setup_inputs(seed: int = 0) -> dict:
    seeds = jax.random.split(jax.random.key(seed), 10)
    return {
        "table": scatter_about(seeds[0], (ENTITIES, D), 0.25, 1.5, ((0, 32),)),
        "relations": scatter_about(seeds[1], (NREL, D), 1.0, 6.0),
        "req_rows": draw_req_rows(jax.random.fold_in(seeds[9], 71), 0),
        "owner_count": draw_owner_count(jax.random.fold_in(seeds[9], 71), 0),
        "owner_start": draw_owner_start(jax.random.fold_in(seeds[9], 71), 0),
        "head_slot": draw_head_slot(jax.random.fold_in(seeds[9], 71), 0),
        "rel_id": touch_ends(ranked(seeds[6], (OWNERS * B_DEV,), NREL, 2), jax.random.fold_in(seeds[6], 3), 0, NREL - 1).astype(jnp.int32),
        "tail_slot": draw_tail_slot(jax.random.fold_in(seeds[9], 71), 0),
        "neg_slot": draw_neg_slot(jax.random.fold_in(seeds[9], 71), 0),
    }


def locate(slot_ids, start, count, cap):
    owners = start.shape[0]
    offset = slot_ids[:, None] - start[None, :]
    match = (offset >= 0) & (offset < count[None, :])
    owner_ids = jnp.arange(owners, dtype=jnp.int32)
    flat = jnp.sum(jnp.where(match, owner_ids[None, :] * cap + offset, 0), axis=1).astype(jnp.int32)
    valid = jnp.any(match, axis=1)
    return flat, valid


def slot_gradients(rows, flat, valid, rel_rows, batch):
    emb = jnp.where(valid[:, None], jnp.take(rows, flat, axis=0), jnp.zeros((), jnp.bfloat16))
    head = emb[:batch]
    tail = emb[batch:2 * batch]
    negative = emb[2 * batch:]
    rvec = rel_rows.astype(jnp.float32)
    query = head.astype(jnp.float32) * rvec
    query_half = query.astype(jnp.bfloat16)
    positive = jnp.sum(query * tail.astype(jnp.float32), axis=1)
    negative_score = lax.dot_general(query_half, negative, (((1,), (1,)), ((), ())), preferred_element_type=jnp.float32)
    pos_weight = -jax.nn.sigmoid(-positive)
    neg_weight = jax.nn.sigmoid(negative_score).astype(jnp.bfloat16)
    head_grad = rvec * (pos_weight[:, None] * tail.astype(jnp.float32) + jnp.dot(neg_weight, negative, preferred_element_type=jnp.float32))
    tail_grad = pos_weight[:, None] * query
    neg_grad = lax.dot_general(neg_weight, query_half, (((0,), (0,)), ((), ())), preferred_element_type=jnp.float32)
    per_row = jnp.concatenate([head_grad, tail_grad, neg_grad], axis=0)
    per_row = jnp.where(valid[:, None], per_row, jnp.zeros((), jnp.float32))
    return jax.ops.segment_sum(per_row, flat, num_segments=rows.shape[0])


def reference(table, relations, req_rows, owner_count, owner_start, head_slot, rel_id, tail_slot, neg_slot):
    owners = OWNERS
    cap = CAP
    heads = head_slot.reshape(owners, B_DEV)
    tails = tail_slot.reshape(owners, B_DEV)
    negs = neg_slot.reshape(owners, NEG)
    rels = rel_id.reshape(owners, B_DEV)
    column = jnp.arange(cap, dtype=jnp.int32)
    owner_ids = jnp.arange(owners, dtype=jnp.int32)

    def device(grad, p):
        count = owner_count[p]
        start = owner_start[p]
        packed = req_rows[p]
        live = column[None, :] < count[:, None]
        where_at = jnp.clip(start[:, None] + column[None, :], 0, SLOTS - 1).astype(jnp.int32)
        local = jnp.where(live, jnp.take(packed, where_at), 0).astype(jnp.int32)
        global_ids = (owner_ids[:, None] * ENT_DEV + local).reshape(-1).astype(jnp.int32)
        rows = jnp.where(live.reshape(-1, 1), jnp.take(table, global_ids, axis=0), jnp.zeros((), jnp.bfloat16))
        lookups = jnp.concatenate([heads[p], tails[p], negs[p]]).astype(jnp.int32)
        flat, valid = locate(lookups, start, count, cap)
        rel_rows = jnp.take(relations, rels[p], axis=0)
        grads = slot_gradients(rows, flat, valid, rel_rows, B_DEV)
        return grad.at[global_ids].add(grads), None

    total = jnp.zeros((ENTITIES, D), jnp.float32)
    total, _ = lax.scan(device, total, jnp.arange(owners, dtype=jnp.int32))
    return total
```

```python
import jax
import jax.numpy as jnp
from jax import lax
from jax.sharding import PartitionSpec as P

AXES = ("wide", "narrow")
NN = (((1,), (0,)), ((), ()))
NT = (((1,), (1,)), ((), ()))
TN = (((0,), (0,)), ((), ()))


def mm(a, b, dims):
    return lax.dot_general(a, b, dims, preferred_element_type=jnp.float32)


def exchange(x):
    return lax.all_to_all(x, AXES, split_axis=0, concat_axis=0, tiled=True)


def per_device(
    table, relations, req_rows, owner_count, owner_start, head_slot, rel_id, tail_slot, neg_slot
):
    owners = lax.axis_size("wide") * lax.axis_size("narrow")
    slots = req_rows.shape[1]
    cap = slots // owners
    width = table.shape[1]
    count = owner_count[0]
    start = owner_start[0]
    packed = req_rows[0]
    column = jnp.arange(cap, dtype=jnp.int32)
    live = column[None, :] < count[:, None]
    held = jnp.where(live, start[:, None] + column[None, :], -1)
    slot_ids = jnp.arange(slots, dtype=jnp.int32)
    hit = held[:, :, None] == slot_ids[None, None, :]
    bucket = jnp.sum(jnp.where(hit, packed[None, None, :] + 1, 0), axis=2) - 1
    wanted = exchange(bucket).reshape(-1)
    rel_rows = jnp.take(relations, rel_id, axis=0, mode="clip")

    row_ids = jnp.arange(table.shape[0], dtype=jnp.int32)
    placer = (wanted[:, None] == row_ids[None, :]).astype(jnp.bfloat16)
    found = mm(placer, table, NN).astype(jnp.bfloat16)
    rows = exchange(found.reshape(owners, cap, width)).reshape(slots, width)

    flat = held.reshape(-1)
    head_pick = head_slot[:, None] == flat[None, :]
    tail_pick = tail_slot[:, None] == flat[None, :]
    times = jnp.sum((neg_slot[:, None] == flat[None, :]).astype(jnp.float32), axis=0)
    head_hot = head_pick.astype(jnp.bfloat16)

    rvec = rel_rows.astype(jnp.float32)
    query = (mm(head_hot, rows, NN) * rvec).astype(jnp.bfloat16)
    score = mm(query, rows, NT)
    up = jax.nn.sigmoid(score)
    weight = times[None, :] * up - jnp.where(tail_pick, jax.nn.sigmoid(-score), 0.0)
    weight = weight.astype(jnp.bfloat16)
    head_grad = (mm(weight, rows, NN) * rvec).astype(jnp.bfloat16)
    grads = mm(weight, query, TN) + mm(head_hot, head_grad, TN)
    back = exchange(grads.astype(jnp.bfloat16).reshape(owners, cap, width))
    return mm(placer, back.reshape(slots, width), TN)


def solution(mesh):
    rows = P(AXES, None)
    flat = P(AXES)
    in_specs = (rows, P(), rows, rows, rows, flat, flat, flat, flat)
    return jax.shard_map(per_device, mesh=mesh, in_specs=in_specs, out_specs=rows, check_vma=False)
```

```python
import jax
import jax.numpy as jnp
from jax import lax
from jax.experimental import pallas as pl
from jax.experimental.pallas import tpu as pltpu
from jax.sharding import PartitionSpec as P

AXES = ("wide", "narrow")
NN = (((1,), (0,)), ((), ()))
NT = (((1,), (1,)), ((), ()))
TN = (((0,), (0,)), ((), ()))
LANES = 128
VMEM = pl.BlockSpec(memory_space=pltpu.VMEM)
HBM = pl.BlockSpec(memory_space=pltpu.HBM)
BF = jnp.bfloat16
F32 = jnp.float32
I32 = jnp.int32


def mm(a, b, dims):
    return lax.dot_general(a, b, dims, preferred_element_type=F32)


def exchange(x):
    return lax.all_to_all(x, AXES, split_axis=0, concat_axis=0, tiled=True)


def iota(shape, dim):
    return lax.broadcasted_iota(I32, shape, dim)


def request_kernel(
    cap, packed_hbm, count_hbm, start_hbm, bucket_ref, held_ref, packed_ref, count_ref, start_ref, sems
):
    copies = [
        pltpu.make_async_copy(count_hbm, count_ref, sems.at[0]),
        pltpu.make_async_copy(start_hbm, start_ref, sems.at[1]),
        pltpu.make_async_copy(packed_hbm, packed_ref, sems.at[2]),
    ]
    for copy in copies:
        copy.start()
    for copy in copies:
        copy.wait()
    owners = bucket_ref.shape[0]
    slots = packed_ref.shape[1]

    def column(ref):
        spread = jnp.broadcast_to(ref[...], (owners, owners))
        diagonal = iota((owners, owners), 0) == iota((owners, owners), 1)
        return jnp.sum(jnp.where(diagonal, spread, 0), axis=1, keepdims=True)

    lane = iota((owners, LANES), 1)
    held = jnp.where(lane < jnp.minimum(column(count_ref), cap), column(start_ref) + lane, -1)
    held_ref[...] = held
    at = jnp.bitwise_and(held, LANES - 1)
    block = jnp.right_shift(held, 7)
    bucket = jnp.full((owners, LANES), -1, I32)
    for j in range(slots // LANES):
        source = jnp.broadcast_to(packed_ref[:, j * LANES : (j + 1) * LANES], (owners, LANES))
        picked = jnp.take_along_axis(source, at, axis=1)
        bucket = jnp.where(block == j, picked, bucket)
    bucket_ref[...] = bucket


def fetch_kernel(cap, wanted_ref, table_hbm, found_ref, table_ref, placer_ref, sem):
    copy = pltpu.make_async_copy(table_hbm, table_ref, sem)
    copy.start()
    owners = wanted_ref.shape[0]
    rows = table_ref.shape[0]
    turned = jnp.transpose(wanted_ref[...])
    row_id = iota((cap, rows), 1)
    for o in range(owners):
        wanted = turned[:cap, o : o + 1]
        placer_ref[o * cap : (o + 1) * cap, :] = jnp.where(wanted == row_id, 1.0, 0.0).astype(BF)
    copy.wait()
    found_ref[...] = mm(placer_ref[...], table_ref[...], NN).astype(BF)


def grad_kernel(
    cap, chunk, rows_ref, rel_ref, held_ref, flat_ref, head_ref, head_tile_ref, tail_tile_ref,
    times_ref, out_ref, head_t_ref, q_ref, w_ref, h_ref
):
    batch = rel_ref.shape[0]
    slots = rows_ref.shape[0]
    owners = held_ref.shape[0]
    held_t = jnp.transpose(held_ref[...])
    heads = head_ref[...]
    for o in range(owners):
        same = held_t[:cap, o : o + 1] == heads
        head_t_ref[o * cap : (o + 1) * cap, :] = jnp.where(same, 1.0, 0.0).astype(BF)
    head_cols = jnp.transpose(head_tile_ref[...])
    tail_cols = jnp.transpose(tail_tile_ref[...])
    flat = flat_ref[...]
    times = times_ref[...]
    rows = rows_ref[...]

    def pick(cols, i):
        parts = range(i * chunk // LANES, (i + 1) * chunk // LANES)
        return jnp.concatenate([cols[:, j : j + 1] for j in parts], axis=0) == flat

    for i in range(batch // chunk):
        at = pl.ds(i * chunk, chunk)
        rel = rel_ref[at, :].astype(F32)
        head_hot = jnp.where(pick(head_cols, i), 1.0, 0.0).astype(BF)
        query = (mm(head_hot, rows, NN) * rel).astype(BF)
        q_ref[at, :] = query
        score = mm(query, rows, NT)
        small = jnp.exp(-jnp.abs(score))
        big_part = 1.0 / (1.0 + small)
        small_part = small * big_part
        rising = score >= 0.0
        up = jnp.where(rising, big_part, small_part)
        down = jnp.where(rising, small_part, big_part)
        weight = (times * up - jnp.where(pick(tail_cols, i), down, 0.0)).astype(BF)
        w_ref[at, :] = weight
        h_ref[at, :] = (mm(weight, rows, NN) * rel).astype(BF)
    step = 256 if slots % 256 == 0 else slots
    for j in range(slots // step):
        at = pl.ds(j * step, step)
        total = mm(w_ref[:, at], q_ref[...], TN) + mm(head_t_ref[at, :], h_ref[...], NN)
        out_ref[at, :] = total.astype(BF)


def place_kernel(placer_t_ref, back_ref, out_ref):
    size = out_ref.shape[0]
    at = pl.ds(pl.program_id(0) * size, size)
    out_ref[...] = mm(placer_t_ref[at, :], back_ref[...], NN)


def in_hbm(x):
    return pltpu.with_memory_space_constraint(x, pltpu.HBM)


def shape(dims, dtype):
    return jax.ShapeDtypeStruct(dims, dtype)


def grant(*arrays):
    total = sum(x.size * x.dtype.itemsize for x in arrays)
    return pltpu.CompilerParams(vmem_limit_bytes=2 * total + (4 << 20))


def per_device(
    table, relations, req_rows, owner_count, owner_start, head_slot, rel_id, tail_slot, neg_slot
):
    owners = lax.axis_size("wide") * lax.axis_size("narrow")
    slots = req_rows.shape[1]
    cap = slots // owners
    held_rows, width = table.shape
    batch = head_slot.shape[0]

    bucket, held = pl.pallas_call(
        lambda *refs: request_kernel(cap, *refs),
        name="request",
        out_shape=[shape((owners, LANES), I32)] * 2,
        in_specs=[HBM] * 3,
        out_specs=[VMEM] * 2,
        scratch_shapes=[
            pltpu.VMEM((1, slots), I32),
            pltpu.VMEM((1, owners), I32),
            pltpu.VMEM((1, owners), I32),
            pltpu.SemaphoreType.DMA((3,)),
        ],
        compiler_params=grant(req_rows),
    )(*map(in_hbm, (req_rows, owner_count, owner_start)))
    wanted = exchange(bucket)
    found = pl.pallas_call(
        lambda *refs: fetch_kernel(cap, *refs),
        name="fetch",
        out_shape=shape((slots, width), BF),
        in_specs=[VMEM, HBM],
        out_specs=VMEM,
        scratch_shapes=[
            pltpu.VMEM((held_rows, width), BF),
            pltpu.VMEM((slots, held_rows), BF),
            pltpu.SemaphoreType.DMA,
        ],
        compiler_params=grant(table, shape((slots, held_rows), BF)),
    )(wanted, in_hbm(table))
    rows = exchange(found.reshape(owners, cap, width)).reshape(slots, width)

    rel_rows = jnp.take(relations, rel_id, axis=0, mode="clip")
    flat = held[:, :cap].reshape(-1)
    times = jnp.sum((neg_slot[:, None] == flat[None, :]).astype(F32), axis=0)[None, :]
    row_ids = jnp.arange(held_rows, dtype=I32)
    placer_t = (row_ids[:, None] == wanted[:, :cap].reshape(-1)[None, :]).astype(BF)

    rows, placer_t = lax.optimization_barrier((rows, placer_t))
    square = shape((batch, slots), BF)
    grads = pl.pallas_call(
        lambda *refs: grad_kernel(cap, 2 * LANES, *refs),
        name="grads",
        out_shape=shape((slots, width), BF),
        in_specs=[VMEM] * 8,
        out_specs=VMEM,
        compiler_params=grant(square, square, square, rel_rows, rel_rows, rel_rows),
        scratch_shapes=[
            pltpu.VMEM((slots, batch), BF),
            pltpu.VMEM((batch, width), BF),
            pltpu.VMEM((batch, slots), BF),
            pltpu.VMEM((batch, width), BF),
        ],
    )(
        rows,
        rel_rows,
        held,
        flat[None, :],
        head_slot[None, :],
        head_slot.reshape(-1, LANES),
        tail_slot.reshape(-1, LANES),
        times,
    )
    back = exchange(grads.reshape(owners, cap, width)).reshape(slots, width)
    block = 256 if held_rows % 256 == 0 else held_rows
    return pl.pallas_call(
        place_kernel,
        name="place",
        grid=(held_rows // block,),
        out_shape=shape((held_rows, width), F32),
        in_specs=[VMEM] * 2,
        out_specs=pl.BlockSpec((block, width), lambda i: (i, 0)),
        compiler_params=grant(placer_t, back),
    )(placer_t, back)


def solution(mesh):
    rows = P(AXES, None)
    flat = P(AXES)
    in_specs = (rows, P(), rows, rows, rows, flat, flat, flat, flat)
    return jax.shard_map(per_device, mesh=mesh, in_specs=in_specs, out_specs=rows, check_vma=False)
```

```python
import jax
import jax.numpy as jnp
from jax import lax
from jax.experimental import pallas as pl
from jax.experimental.pallas import tpu as pltpu
from jax.sharding import PartitionSpec as P

AXES = ("wide", "narrow")
NN = (((1,), (0,)), ((), ()))
NT = (((1,), (1,)), ((), ()))
TN = (((0,), (0,)), ((), ()))
LANES = 128
VMEM = pl.BlockSpec(memory_space=pltpu.VMEM)
HBM = pl.BlockSpec(memory_space=pltpu.HBM)
BF = jnp.bfloat16
F32 = jnp.float32
I32 = jnp.int32


def mm(a, b, dims):
    return lax.dot_general(a, b, dims, preferred_element_type=F32)


def exchange(x):
    return lax.all_to_all(x, AXES, split_axis=0, concat_axis=0, tiled=True)


def iota(shape, dim):
    return lax.broadcasted_iota(I32, shape, dim)


def request_kernel(
    cap, packed_hbm, count_hbm, start_hbm, table_hbm, bucket_ref, held_ref, table_ref,
    packed_ref, count_ref, start_ref, sems
):
    copies = [
        pltpu.make_async_copy(count_hbm, count_ref, sems.at[0]),
        pltpu.make_async_copy(start_hbm, start_ref, sems.at[1]),
        pltpu.make_async_copy(packed_hbm, packed_ref, sems.at[2]),
        pltpu.make_async_copy(table_hbm, table_ref, sems.at[3]),
    ]
    for copy in copies:
        copy.start()
    for copy in copies[:3]:
        copy.wait()
    owners = bucket_ref.shape[0]
    slots = packed_ref.shape[1]

    def column(ref):
        spread = jnp.broadcast_to(ref[...], (owners, owners))
        diagonal = iota((owners, owners), 0) == iota((owners, owners), 1)
        return jnp.sum(jnp.where(diagonal, spread, 0), axis=1, keepdims=True)

    lane = iota((owners, LANES), 1)
    held = jnp.where(lane < jnp.minimum(column(count_ref), cap), column(start_ref) + lane, -1)
    held_ref[...] = held
    at = jnp.bitwise_and(held, LANES - 1)
    block = jnp.right_shift(held, 7)
    bucket = jnp.full((owners, LANES), -1, I32)
    for j in range(slots // LANES):
        source = jnp.broadcast_to(packed_ref[:, j * LANES : (j + 1) * LANES], (owners, LANES))
        picked = jnp.take_along_axis(source, at, axis=1)
        bucket = jnp.where(block == j, picked, bucket)
    bucket_ref[...] = bucket
    copies[3].wait()


def fetch_kernel(cap, wanted_ref, table_ref, found_hbm, placer_ref, found_ref, sems):
    owners = wanted_ref.shape[0]
    rows = table_ref.shape[0]
    parts = sems.shape[0]
    size = owners * cap // parts
    turned = jnp.transpose(wanted_ref[...])
    row_id = iota((cap, rows), 1).astype(jnp.int16)
    one, zero = jnp.ones((), BF), jnp.zeros((), BF)
    copies = []
    for p in range(parts):
        for o in range(p * owners // parts, (p + 1) * owners // parts):
            wanted = jnp.broadcast_to(turned[:cap, o : o + 1], (cap, LANES)).astype(jnp.int16)
            wanted = jnp.concatenate([wanted] * (rows // LANES), axis=1)
            placer_ref[o * cap : (o + 1) * cap, :] = jnp.where(wanted == row_id, one, zero)
        at = pl.ds(p * size, size)
        found_ref[at, :] = mm(placer_ref[at, :], table_ref[...], NN).astype(BF)
        copies.append(pltpu.make_async_copy(found_ref.at[at], found_hbm.at[at], sems.at[p]))
        copies[p].start()
    for copy in copies:
        copy.wait()


def grad_kernel(
    cap, chunk, rows_ref, rel_ref, held_ref, flat_ref, head_ref, head_tile_ref, tail_tile_ref,
    times_ref, out_ref, head_t_ref, q_ref, w_ref, h_ref
):
    batch = rel_ref.shape[0]
    slots = rows_ref.shape[0]
    owners = held_ref.shape[0]
    held_t = jnp.transpose(held_ref[...])
    heads = head_ref[...]
    for o in range(owners):
        same = held_t[:cap, o : o + 1] == heads
        head_t_ref[o * cap : (o + 1) * cap, :] = jnp.where(same, 1.0, 0.0).astype(BF)
    head_cols = jnp.transpose(head_tile_ref[...])
    tail_cols = jnp.transpose(tail_tile_ref[...])
    flat = flat_ref[...]
    times = times_ref[...]
    rows = rows_ref[...]

    def pick(cols, i):
        parts = range(i * chunk // LANES, (i + 1) * chunk // LANES)
        return jnp.concatenate([cols[:, j : j + 1] for j in parts], axis=0) == flat

    def score_of(i):
        at = pl.ds(i * chunk, chunk)
        head_hot = jnp.where(pick(head_cols, i), 1.0, 0.0).astype(BF)
        query = (mm(head_hot, rows, NN) * rel_ref[at, :].astype(F32)).astype(BF)
        q_ref[at, :] = query
        return mm(query, rows, NT)

    def sigmoid(x):
        return 1.0 / (1.0 + jnp.exp(-jnp.maximum(x, -87.0)))

    score = score_of(0)
    for i in range(batch // chunk):
        ahead = score_of(i + 1) if (i + 1) * chunk < batch else None
        at = pl.ds(i * chunk, chunk)
        tail = pick(tail_cols, i)
        positive = jnp.sum(jnp.where(tail, score, 0.0), axis=1, keepdims=True)
        weight = times * sigmoid(score)
        weight = jnp.where(tail, weight - sigmoid(-positive), weight).astype(BF)
        w_ref[at, :] = weight
        h_ref[at, :] = (mm(weight, rows, NN) * rel_ref[at, :].astype(F32)).astype(BF)
        score = ahead
    step = 256 if slots % 256 == 0 else slots
    for j in range(slots // step):
        at = pl.ds(j * step, step)
        total = mm(w_ref[:, at], q_ref[...], TN) + mm(head_t_ref[at, :], h_ref[...], NN)
        out_ref[at, :] = total.astype(BF)


def place_kernel(placer_t_ref, back_ref, out_hbm, out_ref, sems):
    parts = sems.shape[0]
    size = out_ref.shape[0] // parts
    copies = []
    for p in range(parts):
        at = pl.ds(p * size, size)
        out_ref[at, :] = mm(placer_t_ref[at, :], back_ref[...], NN)
        copies.append(pltpu.make_async_copy(out_ref.at[at], out_hbm.at[at], sems.at[p]))
        copies[p].start()
    for copy in copies:
        copy.wait()


def in_hbm(x):
    return pltpu.with_memory_space_constraint(x, pltpu.HBM)


def shape(dims, dtype):
    return jax.ShapeDtypeStruct(dims, dtype)


def grant(*arrays):
    total = sum(x.size * x.dtype.itemsize for x in arrays)
    return pltpu.CompilerParams(vmem_limit_bytes=2 * total + (4 << 20))


def per_device(
    table, relations, req_rows, owner_count, owner_start, head_slot, rel_id, tail_slot, neg_slot
):
    owners = lax.axis_size("wide") * lax.axis_size("narrow")
    slots = req_rows.shape[1]
    cap = slots // owners
    held_rows, width = table.shape
    batch = head_slot.shape[0]

    bucket, held, table_here = pl.pallas_call(
        lambda *refs: request_kernel(cap, *refs),
        name="request",
        out_shape=[shape((owners, LANES), I32)] * 2 + [shape(table.shape, BF)],
        in_specs=[HBM] * 4,
        out_specs=[VMEM] * 3,
        scratch_shapes=[
            pltpu.VMEM((1, slots), I32),
            pltpu.VMEM((1, owners), I32),
            pltpu.VMEM((1, owners), I32),
            pltpu.SemaphoreType.DMA((4,)),
        ],
        compiler_params=grant(table),
    )(*map(in_hbm, (req_rows, owner_count, owner_start, table)))
    wanted = exchange(bucket)
    found = pl.pallas_call(
        lambda *refs: fetch_kernel(cap, *refs),
        name="fetch",
        out_shape=shape((slots, width), BF),
        in_specs=[VMEM] * 2,
        out_specs=HBM,
        scratch_shapes=[
            pltpu.VMEM((slots, held_rows), BF),
            pltpu.VMEM((slots, width), BF),
            pltpu.SemaphoreType.DMA((4,)),
        ],
        compiler_params=grant(table, shape((slots, held_rows), BF), shape((slots, width), BF)),
    )(wanted, table_here)
    rows = exchange(found.reshape(owners, cap, width)).reshape(slots, width)

    rel_rows = jnp.take(relations, rel_id, axis=0, mode="clip")
    flat = held[:, :cap].reshape(-1)
    times = jnp.sum((neg_slot[:, None] == flat[None, :]).astype(F32), axis=0)[None, :]
    row_ids = jnp.arange(held_rows, dtype=I32)
    placer_t = (row_ids[:, None] == wanted[:, :cap].reshape(-1)[None, :]).astype(BF)

    rows, placer_t = lax.optimization_barrier((rows, placer_t))
    square = shape((batch, slots), BF)
    grads = pl.pallas_call(
        lambda *refs: grad_kernel(cap, 4 * LANES, *refs),
        name="grads",
        out_shape=shape((slots, width), BF),
        in_specs=[VMEM] * 8,
        out_specs=VMEM,
        compiler_params=grant(square, square, square, square, rel_rows, rel_rows, rel_rows),
        scratch_shapes=[
            pltpu.VMEM((slots, batch), BF),
            pltpu.VMEM((batch, width), BF),
            pltpu.VMEM((batch, slots), BF),
            pltpu.VMEM((batch, width), BF),
        ],
    )(
        rows,
        rel_rows,
        held,
        flat[None, :],
        head_slot[None, :],
        head_slot.reshape(-1, LANES),
        tail_slot.reshape(-1, LANES),
        times,
    )
    back = exchange(grads.reshape(owners, cap, width)).reshape(slots, width)
    return pl.pallas_call(
        place_kernel,
        name="place",
        out_shape=shape((held_rows, width), F32),
        in_specs=[VMEM] * 2,
        out_specs=HBM,
        scratch_shapes=[pltpu.VMEM((held_rows, width), F32), pltpu.SemaphoreType.DMA((8,))],
        compiler_params=grant(placer_t, back, shape((held_rows, width), F32)),
    )(placer_t, back)


def solution(mesh):
    rows = P(AXES, None)
    flat = P(AXES)
    in_specs = (rows, P(), rows, rows, rows, flat, flat, flat, flat)
    return jax.shard_map(per_device, mesh=mesh, in_specs=in_specs, out_specs=rows, check_vma=False)
```

```python
import jax
import jax.numpy as jnp
from jax import lax
from jax.experimental import pallas as pl
from jax.experimental.pallas import tpu as pltpu
from jax.sharding import PartitionSpec as P

AXES = ("wide", "narrow")
NN = (((1,), (0,)), ((), ()))
NT = (((1,), (1,)), ((), ()))
TN = (((0,), (0,)), ((), ()))
LANES = 128
LOG2_E = 1.4426950408889634
VMEM = pl.BlockSpec(memory_space=pltpu.VMEM)
HBM = pl.BlockSpec(memory_space=pltpu.HBM)
BF = jnp.bfloat16
F32 = jnp.float32
I32 = jnp.int32


def mm(a, b, dims):
    return lax.dot_general(a, b, dims, preferred_element_type=F32)


def exchange(x):
    return lax.all_to_all(x, AXES, split_axis=0, concat_axis=0, tiled=True)


def iota(shape, dim):
    return lax.broadcasted_iota(I32, shape, dim)


def request_kernel(
    cap, packed_hbm, count_hbm, start_hbm, bucket_ref, held_ref, packed_ref, count_ref, start_ref, sems
):
    copies = [
        pltpu.make_async_copy(count_hbm, count_ref, sems.at[0]),
        pltpu.make_async_copy(start_hbm, start_ref, sems.at[1]),
        pltpu.make_async_copy(packed_hbm, packed_ref, sems.at[2]),
    ]
    for copy in copies:
        copy.start()
    for copy in copies:
        copy.wait()
    owners = bucket_ref.shape[0]
    slots = packed_ref.shape[1]

    def column(ref):
        spread = jnp.broadcast_to(ref[...], (owners, owners))
        diagonal = iota((owners, owners), 0) == iota((owners, owners), 1)
        return jnp.sum(jnp.where(diagonal, spread, 0), axis=1, keepdims=True)

    lane = iota((owners, LANES), 1)
    held = jnp.where(lane < jnp.minimum(column(count_ref), cap), column(start_ref) + lane, -1)
    held_ref[...] = held
    at = jnp.bitwise_and(held, LANES - 1)
    block = jnp.right_shift(held, 7)
    bucket = jnp.full((owners, LANES), -1, I32)
    for j in range(slots // LANES):
        source = jnp.broadcast_to(packed_ref[:, j * LANES : (j + 1) * LANES], (owners, LANES))
        picked = jnp.take_along_axis(source, at, axis=1)
        bucket = jnp.where(block == j, picked, bucket)
    bucket_ref[...] = bucket


def grad_kernel(
    cap, chunk, rows_ref, rel_ref, held_ref, flat_ref, head_ref, head_tile_ref, tail_tile_ref,
    times_ref, out_ref, head_t_ref, q_ref, w_ref, h_ref
):
    batch = rel_ref.shape[0]
    slots = rows_ref.shape[0]
    owners = held_ref.shape[0]
    held_t = jnp.transpose(held_ref[...])
    heads = head_ref[...]
    for o in range(owners):
        same = held_t[:cap, o : o + 1] == heads
        head_t_ref[o * cap : (o + 1) * cap, :] = jnp.where(same, 1.0, 0.0).astype(BF)
    head_cols = jnp.transpose(head_tile_ref[...])
    tail_cols = jnp.transpose(tail_tile_ref[...])
    flat = flat_ref[...]
    times = times_ref[...]
    rows = rows_ref[...]

    def pick(cols, i):
        parts = range(i * chunk // LANES, (i + 1) * chunk // LANES)
        return jnp.concatenate([cols[:, j : j + 1] for j in parts], axis=0) == flat

    flat16 = jnp.broadcast_to(flat, (16, slots)).astype(jnp.int16)
    flat16 = jnp.concatenate([flat16] * (LANES // 16), axis=0)
    one, zero = jnp.ones((), BF), jnp.zeros((), BF)

    def head_hot(i):
        parts = []
        for j in range(i * chunk // LANES, (i + 1) * chunk // LANES):
            slot = jnp.broadcast_to(head_cols[:, j : j + 1], (LANES, LANES)).astype(jnp.int16)
            slot = jnp.concatenate([slot] * (slots // LANES), axis=1)
            parts.append(jnp.where(slot == flat16, one, zero))
        return jnp.concatenate(parts, axis=0)

    def score_of(i):
        at = pl.ds(i * chunk, chunk)
        query = mm(head_hot(i), rows, NN).astype(BF) * rel_ref[at, :]
        q_ref[at, :] = query
        return mm(query, rows, NT)

    def sigmoid(x):
        return 1.0 / (1.0 + jnp.exp2(jnp.minimum(x * -LOG2_E, 125.5)))

    score = score_of(0)
    for i in range(batch // chunk):
        ahead = score_of(i + 1) if (i + 1) * chunk < batch else None
        at = pl.ds(i * chunk, chunk)
        tail = pick(tail_cols, i)
        positive = jnp.sum(jnp.where(tail, score, 0.0), axis=1, keepdims=True)
        weight = times * sigmoid(score)
        weight = jnp.where(tail, weight - sigmoid(-positive), weight).astype(BF)
        w_ref[at, :] = weight
        h_ref[at, :] = (mm(weight, rows, NN) * rel_ref[at, :].astype(F32)).astype(BF)
        score = ahead
    step = 256 if slots % 256 == 0 else slots
    for j in range(slots // step):
        at = pl.ds(j * step, step)
        total = mm(w_ref[:, at], q_ref[...], TN) + mm(head_t_ref[at, :], h_ref[...], NN)
        out_ref[at, :] = total.astype(BF)


def place_kernel(wanted_ref, back_ref, out_hbm, out_ref, sems):
    parts = sems.shape[0]
    size = out_ref.shape[0] // parts
    slots = back_ref.shape[0]
    wanted = jnp.broadcast_to(wanted_ref[...], (16, slots)).astype(jnp.int16)
    wanted = jnp.concatenate([wanted] * (size // 16), axis=0)
    row_id = iota((size, slots), 0)
    one, zero = jnp.ones((), BF), jnp.zeros((), BF)
    copies = []
    for p in range(parts):
        at = pl.ds(p * size, size)
        placer = jnp.where((row_id + p * size).astype(jnp.int16) == wanted, one, zero)
        out_ref[at, :] = mm(placer, back_ref[...], NN)
        copies.append(pltpu.make_async_copy(out_ref.at[at], out_hbm.at[at], sems.at[p]))
        copies[p].start()
    for copy in copies:
        copy.wait()


def in_hbm(x):
    return pltpu.with_memory_space_constraint(x, pltpu.HBM)


def shape(dims, dtype):
    return jax.ShapeDtypeStruct(dims, dtype)


def grant(*arrays):
    total = sum(x.size * x.dtype.itemsize for x in arrays)
    return pltpu.CompilerParams(vmem_limit_bytes=2 * total + (4 << 20))


def per_device(
    table, relations, req_rows, owner_count, owner_start, head_slot, rel_id, tail_slot, neg_slot
):
    owners = lax.axis_size("wide") * lax.axis_size("narrow")
    slots = req_rows.shape[1]
    cap = slots // owners
    held_rows, width = table.shape
    batch = head_slot.shape[0]

    bucket, held = pl.pallas_call(
        lambda *refs: request_kernel(cap, *refs),
        name="request",
        out_shape=[shape((owners, LANES), I32)] * 2,
        in_specs=[HBM] * 3,
        out_specs=[VMEM] * 2,
        scratch_shapes=[
            pltpu.VMEM((1, slots), I32),
            pltpu.VMEM((1, owners), I32),
            pltpu.VMEM((1, owners), I32),
            pltpu.SemaphoreType.DMA((3,)),
        ],
        compiler_params=grant(req_rows),
    )(*map(in_hbm, (req_rows, owner_count, owner_start)))
    wanted = exchange(bucket)
    row_ids = jnp.arange(held_rows, dtype=I32)
    placer = (wanted[:, :cap].reshape(-1)[:, None] == row_ids[None, :]).astype(BF)
    found = mm(placer, table, NN).astype(BF)
    rows = exchange(found.reshape(owners, cap, width)).reshape(slots, width)

    rel_rows = jnp.take(relations, rel_id, axis=0, mode="clip")
    flat = held[:, :cap].reshape(-1)
    times = jnp.sum((neg_slot[:, None] == flat[None, :]).astype(F32), axis=0)[None, :]
    wanted_row = wanted[:, :cap].reshape(1, -1)
    rows, wanted_row = lax.optimization_barrier((rows, wanted_row))
    square = shape((batch, slots), BF)
    grads = pl.pallas_call(
        lambda *refs: grad_kernel(cap, 4 * LANES, *refs),
        name="grads",
        out_shape=shape((slots, width), BF),
        in_specs=[VMEM] * 8,
        out_specs=VMEM,
        compiler_params=grant(square, square, square, square, rel_rows, rel_rows, rel_rows),
        scratch_shapes=[
            pltpu.VMEM((slots, batch), BF),
            pltpu.VMEM((batch, width), BF),
            pltpu.VMEM((batch, slots), BF),
            pltpu.VMEM((batch, width), BF),
        ],
    )(
        rows,
        rel_rows,
        held,
        flat[None, :],
        head_slot[None, :],
        head_slot.reshape(-1, LANES),
        tail_slot.reshape(-1, LANES),
        times,
    )
    back = exchange(grads.reshape(owners, cap, width)).reshape(slots, width)
    return pl.pallas_call(
        place_kernel,
        name="place",
        out_shape=shape((held_rows, width), F32),
        in_specs=[VMEM] * 2,
        out_specs=HBM,
        scratch_shapes=[pltpu.VMEM((held_rows, width), F32), pltpu.SemaphoreType.DMA((8,))],
        compiler_params=grant(back, shape((held_rows, width), F32)),
    )(wanted_row, back)


def solution(mesh):
    rows = P(AXES, None)
    flat = P(AXES)
    in_specs = (rows, P(), rows, rows, rows, flat, flat, flat, flat)
    return jax.shard_map(per_device, mesh=mesh, in_specs=in_specs, out_specs=rows, check_vma=False)
```

```python
import jax
import jax.numpy as jnp
from jax import lax
from jax.experimental import pallas as pl
from jax.experimental.pallas import tpu as pltpu
from jax.sharding import PartitionSpec as P

AXES = ("wide", "narrow")
NN = (((1,), (0,)), ((), ()))
NT = (((1,), (1,)), ((), ()))
TN = (((0,), (0,)), ((), ()))
LANES = 128
LOG2_E = 1.4426950408889634
VMEM = pl.BlockSpec(memory_space=pltpu.VMEM)
HBM = pl.BlockSpec(memory_space=pltpu.HBM)
BF = jnp.bfloat16
F32 = jnp.float32
I32 = jnp.int32


def mm(a, b, dims):
    return lax.dot_general(a, b, dims, preferred_element_type=F32)


def exchange(x):
    return lax.all_to_all(x, AXES, split_axis=0, concat_axis=0, tiled=True)


def iota(shape, dim):
    return lax.broadcasted_iota(I32, shape, dim)


def request_kernel(
    cap, packed_hbm, count_hbm, start_hbm, bucket_ref, held_ref, packed_ref, count_ref, start_ref, sems
):
    copies = [
        pltpu.make_async_copy(count_hbm, count_ref, sems.at[0]),
        pltpu.make_async_copy(start_hbm, start_ref, sems.at[1]),
        pltpu.make_async_copy(packed_hbm, packed_ref, sems.at[2]),
    ]
    for copy in copies:
        copy.start()
    copies[0].wait()
    copies[1].wait()
    owners = bucket_ref.shape[0]
    slots = packed_ref.shape[1]

    def column(ref):
        spread = jnp.broadcast_to(ref[...], (owners, owners))
        diagonal = iota((owners, owners), 0) == iota((owners, owners), 1)
        return jnp.sum(jnp.where(diagonal, spread, 0), axis=1, keepdims=True)

    lane = iota((owners, LANES), 1)
    held = jnp.where(lane < jnp.minimum(column(count_ref), cap), column(start_ref) + lane, -1)
    held_ref[...] = held
    at = jnp.bitwise_and(held, LANES - 1)
    block = jnp.right_shift(held, 7)
    copies[2].wait()
    bucket = jnp.full((owners, LANES), -1, I32)
    for j in range(slots // LANES):
        source = jnp.broadcast_to(packed_ref[:, j * LANES : (j + 1) * LANES], (owners, LANES))
        picked = jnp.take_along_axis(source, at, axis=1)
        bucket = jnp.where(block == j, picked, bucket)
    bucket_ref[...] = bucket


def grad_kernel(
    cap, chunk, rows_ref, rel_ref, held_ref, flat_ref, head_ref, head_tile_ref, tail_tile_ref,
    times_ref, out_ref, head_t_ref, q_ref, w_ref, h_ref
):
    batch = rel_ref.shape[0]
    slots = rows_ref.shape[0]
    owners = held_ref.shape[0]
    held_t = jnp.transpose(held_ref[...])
    heads = head_ref[...]
    for o in range(owners):
        same = held_t[:cap, o : o + 1] == heads
        head_t_ref[o * cap : (o + 1) * cap, :] = jnp.where(same, 1.0, 0.0).astype(BF)
    head_cols = jnp.transpose(head_tile_ref[...])
    tail_cols = jnp.transpose(tail_tile_ref[...])
    flat = flat_ref[...]
    times = times_ref[...]
    rows = rows_ref[...]

    def pick(cols, i):
        parts = range(i * chunk // LANES, (i + 1) * chunk // LANES)
        return jnp.concatenate([cols[:, j : j + 1] for j in parts], axis=0) == flat

    flat16 = jnp.broadcast_to(flat, (16, slots)).astype(jnp.int16)
    flat16 = jnp.concatenate([flat16] * (LANES // 16), axis=0)
    one, zero = jnp.ones((), BF), jnp.zeros((), BF)

    def head_hot(i):
        parts = []
        for j in range(i * chunk // LANES, (i + 1) * chunk // LANES):
            slot = jnp.broadcast_to(head_cols[:, j : j + 1], (LANES, LANES)).astype(jnp.int16)
            slot = jnp.concatenate([slot] * (slots // LANES), axis=1)
            parts.append(jnp.where(slot == flat16, one, zero))
        return jnp.concatenate(parts, axis=0)

    def score_of(i):
        at = pl.ds(i * chunk, chunk)
        query = mm(head_hot(i), rows, NN).astype(BF) * rel_ref[at, :]
        q_ref[at, :] = query
        return mm(query, rows, NT)

    def sigmoid(x):
        return 1.0 / (1.0 + jnp.exp2(jnp.minimum(x * -LOG2_E, 125.5)))

    score = score_of(0)
    for i in range(batch // chunk):
        ahead = score_of(i + 1) if (i + 1) * chunk < batch else None
        at = pl.ds(i * chunk, chunk)
        tail = pick(tail_cols, i)
        positive = jnp.sum(jnp.where(tail, score, 0.0), axis=1, keepdims=True)
        weight = times * sigmoid(score)
        weight = jnp.where(tail, weight - sigmoid(-positive), weight).astype(BF)
        w_ref[at, :] = weight
        h_ref[at, :] = (mm(weight, rows, NN) * rel_ref[at, :].astype(F32)).astype(BF)
        score = ahead
    step = 256 if slots % 256 == 0 else slots
    for j in range(slots // step):
        at = pl.ds(j * step, step)
        total = mm(w_ref[:, at], q_ref[...], TN) + mm(head_t_ref[at, :], h_ref[...], NN)
        out_ref[at, :] = total.astype(BF)


def place_kernel(wanted_ref, back_ref, out_hbm, out_ref, sems):
    parts = sems.shape[0]
    size = out_ref.shape[0] // parts
    slots = back_ref.shape[0]
    wanted = jnp.broadcast_to(wanted_ref[...], (16, slots)).astype(jnp.int16)
    wanted = jnp.concatenate([wanted] * (size // 16), axis=0)
    row_id = iota((size, slots), 0)
    one, zero = jnp.ones((), BF), jnp.zeros((), BF)
    copies = []
    for p in range(parts):
        at = pl.ds(p * size, size)
        placer = jnp.where((row_id + p * size).astype(jnp.int16) == wanted, one, zero)
        out_ref[at, :] = mm(placer, back_ref[...], NN)
        copies.append(pltpu.make_async_copy(out_ref.at[at], out_hbm.at[at], sems.at[p]))
        copies[p].start()
    for copy in copies:
        copy.wait()


def in_hbm(x):
    return pltpu.with_memory_space_constraint(x, pltpu.HBM)


def shape(dims, dtype):
    return jax.ShapeDtypeStruct(dims, dtype)


def grant(*arrays):
    total = sum(x.size * x.dtype.itemsize for x in arrays)
    return pltpu.CompilerParams(vmem_limit_bytes=2 * total + (4 << 20))


def per_device(
    table, relations, req_rows, owner_count, owner_start, head_slot, rel_id, tail_slot, neg_slot
):
    owners = lax.axis_size("wide") * lax.axis_size("narrow")
    slots = req_rows.shape[1]
    cap = slots // owners
    held_rows, width = table.shape
    batch = head_slot.shape[0]

    bucket, held = pl.pallas_call(
        lambda *refs: request_kernel(cap, *refs),
        name="request",
        out_shape=[shape((owners, LANES), I32)] * 2,
        in_specs=[HBM] * 3,
        out_specs=[VMEM] * 2,
        scratch_shapes=[
            pltpu.VMEM((1, slots), I32),
            pltpu.VMEM((1, owners), I32),
            pltpu.VMEM((1, owners), I32),
            pltpu.SemaphoreType.DMA((3,)),
        ],
        compiler_params=grant(req_rows),
    )(*map(in_hbm, (req_rows, owner_count, owner_start)))
    wanted = exchange(bucket)
    row_ids = jnp.arange(held_rows, dtype=I32)
    placer = (wanted[:, :cap].reshape(-1)[:, None] == row_ids[None, :]).astype(BF)
    found = mm(placer, table, NN).astype(BF)
    rows = exchange(found.reshape(owners, cap, width)).reshape(slots, width)

    rel_rows = jnp.take(relations, rel_id, axis=0, mode="clip")
    flat = held[:, :cap].reshape(-1)
    times = jnp.sum((neg_slot[:, None] == flat[None, :]).astype(F32), axis=0)[None, :]
    wanted_row = wanted[:, :cap].reshape(1, -1)
    rows, wanted_row = lax.optimization_barrier((rows, wanted_row))
    square = shape((batch, slots), BF)
    grads = pl.pallas_call(
        lambda *refs: grad_kernel(cap, 4 * LANES, *refs),
        name="grads",
        out_shape=shape((slots, width), BF),
        in_specs=[VMEM] * 8,
        out_specs=VMEM,
        compiler_params=grant(square, square, square, square, rel_rows, rel_rows, rel_rows),
        scratch_shapes=[
            pltpu.VMEM((slots, batch), BF),
            pltpu.VMEM((batch, width), BF),
            pltpu.VMEM((batch, slots), BF),
            pltpu.VMEM((batch, width), BF),
        ],
    )(
        rows,
        rel_rows,
        held,
        flat[None, :],
        head_slot[None, :],
        head_slot.reshape(-1, LANES),
        tail_slot.reshape(-1, LANES),
        times,
    )
    back = exchange(grads.reshape(owners, cap, width)).reshape(slots, width)
    return pl.pallas_call(
        place_kernel,
        name="place",
        out_shape=shape((held_rows, width), F32),
        in_specs=[VMEM] * 2,
        out_specs=HBM,
        scratch_shapes=[pltpu.VMEM((held_rows, width), F32), pltpu.SemaphoreType.DMA((8,))],
        compiler_params=grant(back, shape((held_rows, width), F32)),
    )(wanted_row, back)


def solution(mesh):
    rows = P(AXES, None)
    flat = P(AXES)
    in_specs = (rows, P(), rows, rows, rows, flat, flat, flat, flat)
    return jax.shard_map(per_device, mesh=mesh, in_specs=in_specs, out_specs=rows, check_vma=False)
```

```python
import jax
import jax.numpy as jnp
from jax import lax
from jax.experimental import pallas as pl
from jax.experimental.pallas import tpu as pltpu
from jax.sharding import PartitionSpec as P

AXES = ("wide", "narrow")
NN = (((1,), (0,)), ((), ()))
NT = (((1,), (1,)), ((), ()))
TN = (((0,), (0,)), ((), ()))
LANES = 128
LOG2_E = 1.4426950408889634
VMEM = pl.BlockSpec(memory_space=pltpu.VMEM)
HBM = pl.BlockSpec(memory_space=pltpu.HBM)
BF = jnp.bfloat16
F32 = jnp.float32
I32 = jnp.int32


def mm(a, b, dims):
    return lax.dot_general(a, b, dims, preferred_element_type=F32)


def exchange(x):
    return lax.all_to_all(x, AXES, split_axis=0, concat_axis=0, tiled=True)


def iota(shape, dim):
    return lax.broadcasted_iota(I32, shape, dim)


def request_kernel(
    cap, packed_hbm, count_hbm, start_hbm, bucket_ref, held_ref, packed_ref, count_ref, start_ref, sems
):
    copies = [
        pltpu.make_async_copy(count_hbm, count_ref, sems.at[0]),
        pltpu.make_async_copy(start_hbm, start_ref, sems.at[1]),
        pltpu.make_async_copy(packed_hbm, packed_ref, sems.at[2]),
    ]
    for copy in copies:
        copy.start()
    copies[0].wait()
    copies[1].wait()
    owners = bucket_ref.shape[0]
    slots = packed_ref.shape[1]

    def column(ref):
        spread = jnp.broadcast_to(ref[...], (owners, owners))
        diagonal = iota((owners, owners), 0) == iota((owners, owners), 1)
        return jnp.sum(jnp.where(diagonal, spread, 0), axis=1, keepdims=True)

    lane = iota((owners, LANES), 1)
    held = jnp.where(lane < jnp.minimum(column(count_ref), cap), column(start_ref) + lane, -1)
    held_ref[...] = held
    at = jnp.bitwise_and(held, LANES - 1)
    block = jnp.right_shift(held, 7)
    copies[2].wait()
    bucket = jnp.full((owners, LANES), -1, I32)
    for j in range(slots // LANES):
        source = jnp.broadcast_to(packed_ref[:, j * LANES : (j + 1) * LANES], (owners, LANES))
        picked = jnp.take_along_axis(source, at, axis=1)
        bucket = jnp.where(block == j, picked, bucket)
    bucket_ref[...] = bucket


def grad_kernel(
    cap, chunk, rows_ref, rel_ref, held_ref, flat_ref, head_ref, head_tile_ref, tail_tile_ref,
    times_ref, out_ref, head_t_ref, q_ref, w_ref, h_ref
):
    batch = rel_ref.shape[0]
    slots = rows_ref.shape[0]
    owners = held_ref.shape[0]
    held_t = jnp.transpose(held_ref[...])
    heads = head_ref[...]
    for o in range(owners):
        same = held_t[:cap, o : o + 1] == heads
        head_t_ref[o * cap : (o + 1) * cap, :] = jnp.where(same, 1.0, 0.0).astype(BF)
    head_cols = jnp.transpose(head_tile_ref[...])
    tail_cols = jnp.transpose(tail_tile_ref[...])
    flat = flat_ref[...]
    times = times_ref[...]
    rows = rows_ref[...]

    def pick(cols, i):
        parts = range(i * chunk // LANES, (i + 1) * chunk // LANES)
        return jnp.concatenate([cols[:, j : j + 1] for j in parts], axis=0) == flat

    flat16 = jnp.broadcast_to(flat, (16, slots)).astype(jnp.int16)
    flat16 = jnp.concatenate([flat16] * (LANES // 16), axis=0)
    one, zero = jnp.ones((), BF), jnp.zeros((), BF)

    def head_hot(i):
        parts = []
        for j in range(i * chunk // LANES, (i + 1) * chunk // LANES):
            slot = jnp.broadcast_to(head_cols[:, j : j + 1], (LANES, LANES)).astype(jnp.int16)
            slot = jnp.concatenate([slot] * (slots // LANES), axis=1)
            parts.append(jnp.where(slot == flat16, one, zero))
        return jnp.concatenate(parts, axis=0)

    def score_of(i):
        at = pl.ds(i * chunk, chunk)
        query = mm(head_hot(i), rows, NN).astype(BF) * rel_ref[at, :]
        q_ref[at, :] = query
        return mm(query, rows, NT)

    def sigmoid(x):
        return 1.0 / (1.0 + jnp.exp2(jnp.minimum(x * -LOG2_E, 125.5)))

    score = score_of(0)
    for i in range(batch // chunk):
        ahead = score_of(i + 1) if (i + 1) * chunk < batch else None
        at = pl.ds(i * chunk, chunk)
        tail = pick(tail_cols, i)
        positive = jnp.sum(jnp.where(tail, score, 0.0), axis=1, keepdims=True)
        weight = times * sigmoid(score)
        weight = jnp.where(tail, weight - sigmoid(-positive), weight).astype(BF)
        w_ref[at, :] = weight
        h_ref[at, :] = (mm(weight, rows, NN) * rel_ref[at, :].astype(F32)).astype(BF)
        score = ahead
    step = 256 if slots % 256 == 0 else slots
    for j in range(slots // step):
        at = pl.ds(j * step, step)
        total = mm(w_ref[:, at], q_ref[...], TN) + mm(head_t_ref[at, :], h_ref[...], NN)
        out_ref[at, :] = total.astype(BF)


def place_kernel(wanted_ref, back_ref, out_hbm, out_ref, sems):
    parts = sems.shape[0]
    size = out_ref.shape[0] // parts
    slots = back_ref.shape[0]
    wanted = jnp.broadcast_to(wanted_ref[...], (16, slots)).astype(jnp.int16)
    wanted = jnp.concatenate([wanted] * (size // 16), axis=0)
    row_id = iota((size, slots), 0)
    one, zero = jnp.ones((), BF), jnp.zeros((), BF)
    copies = []
    for p in range(parts):
        at = pl.ds(p * size, size)
        placer = jnp.where((row_id + p * size).astype(jnp.int16) == wanted, one, zero)
        out_ref[at, :] = mm(placer, back_ref[...], NN)
        copies.append(pltpu.make_async_copy(out_ref.at[at], out_hbm.at[at], sems.at[p]))
        copies[p].start()
    for copy in copies:
        copy.wait()


def in_hbm(x):
    return pltpu.with_memory_space_constraint(x, pltpu.HBM)


def shape(dims, dtype):
    return jax.ShapeDtypeStruct(dims, dtype)


def grant(*arrays):
    total = sum(x.size * x.dtype.itemsize for x in arrays)
    return pltpu.CompilerParams(vmem_limit_bytes=2 * total + (4 << 20))


def per_device(
    table, relations, req_rows, owner_count, owner_start, head_slot, rel_id, tail_slot, neg_slot
):
    owners = lax.axis_size("wide") * lax.axis_size("narrow")
    slots = req_rows.shape[1]
    cap = slots // owners
    held_rows, width = table.shape
    batch = head_slot.shape[0]

    bucket, held = pl.pallas_call(
        lambda *refs: request_kernel(cap, *refs),
        name="request",
        out_shape=[shape((owners, LANES), I32)] * 2,
        in_specs=[HBM] * 3,
        out_specs=[VMEM] * 2,
        scratch_shapes=[
            pltpu.VMEM((1, slots), I32),
            pltpu.VMEM((1, owners), I32),
            pltpu.VMEM((1, owners), I32),
            pltpu.SemaphoreType.DMA((3,)),
        ],
        compiler_params=grant(req_rows),
    )(*map(in_hbm, (req_rows, owner_count, owner_start)))
    wanted = exchange(bucket)
    row_ids = jnp.arange(held_rows, dtype=I32)
    placer = (wanted[:, :cap].reshape(-1)[:, None] == row_ids[None, :]).astype(BF)
    found = mm(placer, table, NN).astype(BF)
    rows = exchange(found.reshape(owners, cap, width)).reshape(slots, width)

    rel_rows = jnp.take(relations, rel_id, axis=0, mode="clip")
    flat = held[:, :cap].reshape(-1)
    times = jnp.sum((neg_slot[:, None] == flat[None, :]).astype(F32), axis=0)[None, :]
    wanted_row = wanted[:, :cap].reshape(1, -1)
    rows, wanted_row = lax.optimization_barrier((rows, wanted_row))
    square = shape((batch, slots), BF)
    grads = pl.pallas_call(
        lambda *refs: grad_kernel(cap, 4 * LANES, *refs),
        name="grads",
        out_shape=shape((slots, width), BF),
        in_specs=[VMEM] * 8,
        out_specs=VMEM,
        compiler_params=grant(square, square, square, square, rel_rows, rel_rows, rel_rows),
        scratch_shapes=[
            pltpu.VMEM((slots, batch), BF),
            pltpu.VMEM((batch, width), BF),
            pltpu.VMEM((batch, slots), BF),
            pltpu.VMEM((batch, width), BF),
        ],
    )(
        rows,
        rel_rows,
        held,
        flat[None, :],
        head_slot[None, :],
        head_slot.reshape(-1, LANES),
        tail_slot.reshape(-1, LANES),
        times,
    )
    back = exchange(grads.reshape(owners, cap, width)).reshape(slots, width)
    return pl.pallas_call(
        place_kernel,
        name="place",
        out_shape=shape((held_rows, width), F32),
        in_specs=[VMEM] * 2,
        out_specs=HBM,
        scratch_shapes=[pltpu.VMEM((held_rows, width), F32), pltpu.SemaphoreType.DMA((4,))],
        compiler_params=grant(back, shape((held_rows, width), F32)),
    )(wanted_row, back)


def solution(mesh):
    rows = P(AXES, None)
    flat = P(AXES)
    in_specs = (rows, P(), rows, rows, rows, flat, flat, flat, flat)
    return jax.shard_map(per_device, mesh=mesh, in_specs=in_specs, out_specs=rows, check_vma=False)
```
